256 devices in a mesh: dp: 32 (over y, x, core), tensor: 8 (over z).
Axes of the slice: x: 4, y: 4, z: 8, core: 2. Of those that a mesh axis runs over, the one named last changes fastest.
Arguments:
- queries: bfloat16 [8192, 3072], P('dp', 'tensor'), may hold values from -96 to 96
- keys: bfloat16 [8192, 512], P('dp'), may hold values from -6 to 6
- values: bfloat16 [8192, 512], P('dp'), may hold values from -6 to 6
- lengths: int32 [16], replicated, may hold values from 1 to 6144, 8192 in all
- assignment: int32 [32, 32], replicated, may hold values from 0 to 31, each once within a row
- out_weight: bfloat16 [3072, 6144], P('tensor'), may hold values from -0.109375 to 0.109375
Outputs:
- mixed: bfloat16 [8192, 6144], P(('dp', 'tensor'))
The draws below stay inside these ranges and needn't reach their ends.
Inputs may be any that keep to these rules, and one draw needn't show every extreme that they name: `lengths`: the prompts fill the 8192 positions in order, one of them exactly 6144 long. `assignment`: each row is a permutation of 0 to 31.
All inputs are finite; a program needn't handle non-finite values.
Results may differ from the reference program's by a relative error of at most 0.014.
Values may be sent and summed in bfloat16 or wider, within the bound.
No kernel may reach another device: no remote copies, remote signals or barrier semaphores. Data moves between devices by JAX's collectives and lax.ppermute only.
A program may use at most 64 MiB of HBM per device.

```python
import math
import jax
import jax.numpy as jnp
import numpy as np
from jax import lax

D = 6144
HD = 128
HEADS = 24
KV_HEADS = 4
TOK_DEV = 256
TOKENS = 8192
PIECE = 8
MOST = 6144
DOCS = 16
N_DP = 32
N_TENSOR = 8


def paired_draw(key):
    base = jax.random.fold_in(key, 71)
    key_q, key_k = jax.random.split(base, 2)
    key_vals = jnp.clip(jax.random.normal(key_k, (TOKENS, KV_HEADS, HD), jnp.float32), -4.5, 4.5)
    query_vals = jnp.clip(jax.random.normal(key_q, (TOKENS, HEADS, HD), jnp.float32), -4.5, 4.5)
    return (query_vals.reshape(TOKENS, HEADS * HD), key_vals.reshape(TOKENS, KV_HEADS * HD))


def draw_queries(key, part):
    return paired_draw(key)[0].astype(jnp.bfloat16)


def draw_keys(key, part):
    return paired_draw(key)[1].astype(jnp.bfloat16)


def level_of(rng, dims, shards, smallest, top_value):
    loudness, own = 1.0, jax.random.fold_in(rng, 6)
    for dim, parts in shards:
        heights = jnp.exp(jax.random.uniform(jax.random.fold_in(own, dim), (parts,), jnp.float32, smallest / len(shards), top_value / len(shards)))
        loudness = loudness * jnp.repeat(heights, dims[dim] // parts).reshape([-1 if axis == dim else 1 for axis in range(len(dims))])
    return loudness


def profile(amount, total, limit, skew):
    weights = [(1 << 20) // math.isqrt(standing ** skew) + 1 for standing in range(2, amount + 1)]
    surplus, holding = total - limit - (amount - 1), [1] * (amount - 1)
    while surplus > 0:
        candidates = [i for i in range(amount - 1) if holding[i] < limit]
        pool, left = sum([weights[i] for i in candidates]), surplus
        for i in candidates:
            addition = min(limit - holding[i], max(1, left * weights[i] // pool), surplus)
            holding[i] = holding[i] + addition
            surplus = surplus - addition
    return np.array([limit] + holding)


def ragged_sizes(own_key, amount, total, reach, lean):
    if amount == 2:
        one = jax.random.randint(own_key, (), max(1, total - reach), min(reach, total - 1) + 1)
        return jnp.stack([one, total - one])
    tallies = jnp.asarray(profile(amount, total, reach, lean), jnp.int32)
    twos = (amount - 1) // 2
    giver, taker = tallies[1:1 + 2 * twos:2], tallies[2:2 + 2 * twos:2]
    room = jnp.minimum(giver - 1, reach - taker)
    moved = jax.random.randint(jax.random.fold_in(own_key, 1), (twos,), 0, 1 << 20) % (room + 1)
    tallies = tallies.at[1:1 + 2 * twos:2].set(giver - moved).at[2:2 + 2 * twos:2].set(taker + moved)
    return tallies[jax.random.permutation(jax.random.fold_in(own_key, 2), amount)]


def bell_draw(rng, dims, spread, reach, cuts=(), kind=jnp.bfloat16):
    values = jax.random.normal(rng, dims, jnp.float32) * spread
    if len(cuts) > 0:
        values = level_of(rng, dims, cuts, -0.22, 0.18) * values
    return jnp.clip(values, min=-reach, max=reach).astype(kind)


def setup_inputs(seed: int = 0) -> dict:
    key_of = jax.random.split(jax.random.key(seed), 7)
    queries = draw_queries(jax.random.fold_in(key_of[6], 71), 0)
    keys = draw_keys(jax.random.fold_in(key_of[6], 71), 0)
    values = bell_draw(key_of[2], (TOKENS, KV_HEADS * HD), 1.0, 6.0, ((0, 32),))
    lengths = ragged_sizes(key_of[3], DOCS, TOKENS, MOST, 2).astype(jnp.int32)
    assignment = jax.vmap(lambda own: jax.random.permutation(own, N_DP))(jax.random.split(key_of[4], N_DP)).reshape((N_DP, N_DP)).astype(jnp.int32)
    out_weight = bell_draw(key_of[5], (HEADS * HD, D), (HEADS * HD) ** -0.5, 0.109375, ((0, 8),))
    return {"queries": queries, "keys": keys, "values": values, "lengths": lengths, "assignment": assignment, "out_weight": out_weight}


def reference(queries, keys, values, lengths, assignment, out_weight):
    group_size = HEADS // KV_HEADS
    score_scale = HD ** -0.5
    doc_ends = jnp.cumsum(lengths).astype(jnp.int32)
    places = jnp.arange(TOKENS, dtype=jnp.int32)
    doc_all = jnp.sum((places[:, None] >= doc_ends[None, :]).astype(jnp.int32), axis=1).astype(jnp.int32)
    front_rows = MOST
    key_pad = jnp.concatenate([jnp.zeros((front_rows, KV_HEADS * HD), keys.dtype), keys], axis=0)
    value_pad = jnp.concatenate([jnp.zeros((front_rows, KV_HEADS * HD), values.dtype), values], axis=0)
    doc_pad = jnp.concatenate([jnp.full((front_rows,), -1, jnp.int32), doc_all], axis=0)
    pos_pad = jnp.arange(-front_rows, TOKENS, dtype=jnp.int32)

    def one_block(block_index):
        first_row = (block_index * TOK_DEV).astype(jnp.int32)
        query_rows = lax.dynamic_slice_in_dim(queries, first_row, TOK_DEV, 0).astype(jnp.float32)
        query_rows = query_rows.reshape(TOK_DEV, KV_HEADS, group_size, HD)
        key_rows = lax.dynamic_slice_in_dim(key_pad, first_row, front_rows + TOK_DEV, 0).astype(jnp.float32)
        key_rows = key_rows.reshape(front_rows + TOK_DEV, KV_HEADS, HD)
        value_rows = lax.dynamic_slice_in_dim(value_pad, first_row, front_rows + TOK_DEV, 0).astype(jnp.float32)
        value_rows = value_rows.reshape(front_rows + TOK_DEV, KV_HEADS, HD)
        q_pos = first_row + jnp.arange(TOK_DEV, dtype=jnp.int32)
        q_doc = lax.dynamic_slice_in_dim(doc_all, first_row, TOK_DEV, 0)
        k_pos = lax.dynamic_slice_in_dim(pos_pad, first_row, front_rows + TOK_DEV, 0)
        k_doc = lax.dynamic_slice_in_dim(doc_pad, first_row, front_rows + TOK_DEV, 0)
        visible = (k_doc[None, :] == q_doc[:, None]) & (k_pos[None, :] <= q_pos[:, None])
        scores = jnp.einsum("qcgd,kcd->cgqk", query_rows, key_rows) * score_scale
        scores = jnp.where(visible[None, None], scores, -1e30)
        highest = jnp.max(scores, axis=3)
        weights = jnp.exp(scores - highest[..., None])
        totals = jnp.sum(weights, axis=3)
        rounded = lax.optimization_barrier(weights.astype(jnp.bfloat16))
        summed = jnp.einsum("cgqk,kcd->qcgd", rounded.astype(jnp.float32), value_rows)
        result = summed / jnp.transpose(totals, (2, 0, 1))[..., None]
        return result.reshape(TOK_DEV, HEADS * HD).astype(jnp.bfloat16)

    attended = lax.map(one_block, jnp.arange(N_DP, dtype=jnp.int32))
    attended = attended.reshape(N_DP, N_DP, PIECE, HEADS * HD)
    sources = jnp.arange(N_DP, dtype=jnp.int32)
    regrouped = attended[sources[None, :], jnp.transpose(assignment)]
    regrouped = regrouped.reshape(TOKENS, HEADS * HD)
    lane_cols = HEADS * HD // N_TENSOR
    mixed = jnp.zeros((TOKENS, D), jnp.float32)
    for lane_index in range(N_TENSOR):
        term = jnp.dot(regrouped[:, lane_index * lane_cols:(lane_index + 1) * lane_cols],
                       out_weight[lane_index * lane_cols:(lane_index + 1) * lane_cols],
                       preferred_element_type=jnp.float32)
        term_b = lax.optimization_barrier(term.astype(jnp.bfloat16))
        mixed = mixed + term_b.astype(jnp.float32)
    return mixed.astype(jnp.bfloat16)
```

```python
import functools

import jax
import jax.numpy as jnp
from jax import lax
from jax.experimental import pallas as pl
from jax.experimental.pallas import tpu as pltpu
from jax.sharding import Mesh
from jax.sharding import PartitionSpec as P

HD = 128
HEADS = 24
KV_HEADS = 4
DP = ("dp_0", "dp_1", "dp_2")
DP_TENSOR = ("dp_0", "dp_1", "dp_2", "tensor")
LOG2E = 1.4426950408889634
TILES = 4
BLOCK_K = 512
HIDDEN = -2e30
FLOOR = -1e30


def attention_kernel(
    group_ref, lengths_ref, assignment_ref, q_ref, kv_ref, o_ref, first_ref, last_ref, *, tok_rows
):
    rows = q_ref.shape[0]
    heads = q_ref.shape[1] // HD
    all_rows = kv_ref.shape[0]
    n_groups = assignment_ref.shape[0]
    piece = rows // n_groups
    tile = rows // TILES
    tile_pieces = n_groups // TILES
    factor = HD**-0.5 * LOG2E
    group = group_ref[0]

    ends, at = [], jnp.int32(0)
    for k in range(lengths_ref.shape[0]):
        at = at + lengths_ref[k]
        ends.append(at)

    def place(s):
        return s * tok_rows + assignment_ref[s, group] * piece

    def doc_start(position):
        start = jnp.zeros_like(position)
        for end in ends:
            start = jnp.where(position >= end, end, start)
        return start

    row = lax.broadcasted_iota(jnp.int32, (piece, HD), 0)
    lane = lax.broadcasted_iota(jnp.int32, (heads * tile, HD), 1)

    for t in range(TILES):
        for s in range(t * tile_pieces, (t + 1) * tile_pieces):
            position = place(s) + row
            last_ref[pl.ds(s * piece, piece), :] = position
            first_ref[pl.ds(s * piece, piece), :] = doc_start(position)

    for t in range(TILES):
        low = doc_start(place(t * tile_pieces))
        high = place((t + 1) * tile_pieces - 1) + piece
        low = low // 16 * 16
        count = (high - low + BLOCK_K - 1) // BLOCK_K
        low = jnp.minimum(low, all_rows - count * BLOCK_K)
        span = pl.ds(t * tile, tile)
        q = jnp.concatenate([q_ref[span, h * HD : (h + 1) * HD] for h in range(heads)], axis=0)
        first = jnp.concatenate([first_ref[span, :]] * heads, axis=0)
        last = jnp.concatenate([last_ref[span, :]] * heads, axis=0)

        def step(i, state):
            running, totals, weighted = state
            offset = pl.multiple_of(low + i * BLOCK_K, 16)
            k = kv_ref[pl.ds(offset, BLOCK_K), 0:HD]
            v = kv_ref[pl.ds(offset, BLOCK_K), HD : 2 * HD]
            scores = lax.dot_general(
                q, k, (((1,), (1,)), ((), ())), preferred_element_type=jnp.float32
            )
            parts = []
            for c in range(BLOCK_K // HD):
                position = lane + (offset + c * HD)
                visible = (position >= first) & (position <= last)
                parts.append(jnp.where(visible, scores[:, c * HD : (c + 1) * HD], HIDDEN))
            top = functools.reduce(jnp.maximum, parts)
            highest = jnp.maximum(running, jnp.max(top, axis=1, keepdims=True))
            rescale = jnp.exp2((running - highest) * factor)
            parts = [jnp.exp2((part - highest) * factor) for part in parts]
            totals = totals * rescale + functools.reduce(jnp.add, parts)
            weights = jnp.concatenate([part.astype(jnp.bfloat16) for part in parts], axis=1)
            weighted = weighted * rescale + jnp.dot(weights, v, preferred_element_type=jnp.float32)
            return highest, totals, weighted

        state = (
            jnp.full((heads * tile, 1), FLOOR, jnp.float32),
            jnp.zeros((heads * tile, HD), jnp.float32),
            jnp.zeros((heads * tile, HD), jnp.float32),
        )
        running, totals, weighted = lax.fori_loop(0, count, step, state)
        result = (weighted / jnp.sum(totals, axis=1, keepdims=True)).astype(o_ref.dtype)
        for h in range(heads):
            o_ref[span, h * HD : (h + 1) * HD] = result[h * tile : (h + 1) * tile]


def attention(group, lengths, assignment, q, kv, tok_rows):
    smem = pl.BlockSpec(memory_space=pltpu.SMEM)
    vmem = pl.BlockSpec(memory_space=pltpu.VMEM)
    return pl.pallas_call(
        functools.partial(attention_kernel, tok_rows=tok_rows),
        out_shape=jax.ShapeDtypeStruct(q.shape, q.dtype),
        in_specs=[smem, smem, smem, vmem, vmem],
        out_specs=vmem,
        scratch_shapes=[
            pltpu.VMEM((q.shape[0], HD), jnp.int32),
            pltpu.VMEM((q.shape[0], HD), jnp.int32),
        ],
        cost_estimate=pl.CostEstimate(
            flops=2 * 10**9, bytes_accessed=5 * 10**6, transcendentals=3 * 10**6
        ),
        name="attention",
    )(group, lengths, assignment, q, kv)


def local(queries, keys, values, lengths, assignment, out_weight):
    n_groups = lax.axis_size(DP)
    my_group = lax.axis_index(DP)
    my_lane = lax.axis_index("tensor")
    tok_rows, q_width = queries.shape
    piece = tok_rows // n_groups
    kv_head = my_lane * (q_width // HD) // (HEADS // KV_HEADS)
    own = jnp.concatenate(
        [lax.dynamic_slice_in_dim(a, kv_head * HD, HD, 1) for a in (keys, values)], axis=1
    )
    outgoing = queries.reshape(n_groups, piece, q_width)[assignment[my_group]]
    q = lax.all_to_all(outgoing, DP, 0, 0, tiled=True).reshape(tok_rows, q_width)
    kv = lax.all_gather(own, DP, axis=0, tiled=True)
    group = my_group.astype(jnp.int32).reshape(1)
    attended = attention(group, lengths, assignment, q, kv, tok_rows)
    return lax.psum_scatter(
        jnp.dot(attended, out_weight, preferred_element_type=jnp.float32).astype(jnp.bfloat16),
        "tensor",
        scatter_dimension=0,
        tiled=True,
    )


def solution(mesh):
    split = Mesh(
        mesh.devices.reshape(4, 4, 2, mesh.shape["tensor"]), ("dp_0", "dp_1", "dp_2", "tensor")
    )
    placed = (P(DP, "tensor"), P(DP, None), P(DP, None), P(), P(), P("tensor", None))
    return jax.shard_map(
        local, mesh=split, in_specs=placed, out_specs=P(DP_TENSOR, None), check_vma=False
    )
```

```python
import functools

import jax
import jax.numpy as jnp
from jax import lax
from jax.experimental import pallas as pl
from jax.experimental.pallas import tpu as pltpu
from jax.sharding import Mesh
from jax.sharding import PartitionSpec as P


HD = 128
HEADS = 24
KV_HEADS = 4
DP = ("dp_0", "dp_1", "dp_2")
DP_TENSOR = ("dp_0", "dp_1", "dp_2", "tensor")
LOG2E = 1.4426950408889634
BLOCK_K = 256
UNROLL = 4
COLUMNS = 512
HIDDEN = -2e30
FLOOR = -1e30


def attention_kernel(here_ref, lengths_ref, assignment_ref, q_ref, *refs, slots, lanes, tok_rows):
    sides = 4
    part_refs, weight_ref = refs[: 2 * sides], refs[2 * sides]
    out_refs = refs[2 * sides + 1 : 2 * sides + 1 + 2 * len(slots)]
    scratch = refs[2 * sides + 1 + 2 * len(slots) :]
    kv_ref, w_ref, qs_ref, first_ref, last_ref, scores_ref = scratch[:6]
    top_ref, totals_ref, weighted_ref, o_ref, tile_ref, offset_ref, kv_sem, w_sem = scratch[6:]
    rows = q_ref.shape[0]
    heads = q_ref.shape[1] // HD
    all_rows = kv_ref.shape[0]
    n_groups = assignment_ref.shape[0]
    piece = rows // n_groups
    chunk = rows // lanes
    pieces = n_groups // lanes
    half = tok_rows // 2
    n_tiles = len(slots)
    factor = HD**-0.5 * LOG2E
    y, x, core, my_lane = here_ref[0], here_ref[1], here_ref[2], here_ref[3]
    group = (y * sides + x) * 2 + core

    weight_copy = pltpu.make_async_copy(weight_ref, w_ref, w_sem)
    copies = []
    for swapped in range(2):
        holder = core if swapped == 0 else 1 - core
        along = jnp.where(holder == 0, x, y)
        across = jnp.where(holder == 0, y, x)
        for s in range(sides):
            for r in range(sides):
                u = lax.rem(along + sides - r, sides)
                v = lax.rem(across + sides - s, sides)
                py = jnp.where(holder == 0, v, u)
                px = jnp.where(holder == 0, u, v)
                for k in range(2):
                    source = (py * sides + px) * 2 + k
                    start = pl.multiple_of(source * tok_rows + holder * half, half)
                    begin = (r * 2 + k) * half
                    copies.append(
                        pltpu.make_async_copy(
                            part_refs[swapped * sides + s].at[pl.ds(begin, half), :],
                            kv_ref.at[pl.ds(start, half), :],
                            kv_sem.at[len(copies)],
                        )
                    )
    for copy in copies:
        copy.start()
    weight_copy.start()

    ends, at = [], jnp.int32(0)
    for k in range(lengths_ref.shape[0]):
        at = at + lengths_ref[k]
        ends.append(at)

    def place(s):
        return s * tok_rows + assignment_ref[s, group] * piece

    def doc_start(position):
        start = jnp.zeros_like(position)
        for end in ends:
            start = jnp.where(position >= end, end, start)
        return start

    row = lax.broadcasted_iota(jnp.int32, (piece, HD), 0)
    lane = lax.broadcasted_iota(jnp.int32, (heads * chunk, HD), 1)

    def fill(index, tile, offset):
        tile_ref[index] = tile
        offset_ref[index] = offset

    total = jnp.int32(0)
    for t, slot in enumerate(slots):
        owner = lax.rem(my_lane + slot, lanes)
        low = doc_start(place(owner * pieces)) // 16 * 16
        high = place(owner * pieces + pieces - 1) + piece
        count = (high - low + BLOCK_K - 1) // BLOCK_K
        low = jnp.minimum(low, all_rows - count * BLOCK_K)

        def add(i, carry, t=t, low=low, total=total):
            fill(total + i, t, low + i * BLOCK_K)
            return carry

        lax.fori_loop(0, count, add, 0)
        total = total + count
        begin = pl.multiple_of(owner * chunk, chunk)
        for h in range(heads):
            qs_ref[t, h * chunk : (h + 1) * chunk, :] = q_ref[
                pl.ds(begin, chunk), h * HD : (h + 1) * HD
            ]
        for p in range(pieces):
            position = place(owner * pieces + p) + row
            start = doc_start(position)
            for h in range(heads):
                span = pl.ds(h * chunk + p * piece, piece)
                last_ref[t, span, :] = position
                first_ref[t, span, :] = start
    for u in range(UNROLL - 1):
        fill(total + u, n_tiles, 0)
    steps = (total + UNROLL - 1) // UNROLL
    qs_ref[n_tiles] = jnp.zeros(qs_ref.shape[1:], qs_ref.dtype)
    first_ref[n_tiles] = jnp.ones(first_ref.shape[1:], jnp.int32)
    last_ref[n_tiles] = jnp.zeros(last_ref.shape[1:], jnp.int32)
    top_ref[...] = jnp.full(top_ref.shape, FLOOR, jnp.float32)
    totals_ref[...] = jnp.zeros(totals_ref.shape, jnp.float32)
    weighted_ref[...] = jnp.zeros(weighted_ref.shape, jnp.float32)
    for copy in copies:
        copy.wait()

    def score(i, carry):
        for u in range(UNROLL):
            index = i * UNROLL + u
            t = tile_ref[index]
            offset = pl.multiple_of(offset_ref[index], 16)
            scores = lax.dot_general(
                qs_ref[t],
                kv_ref[pl.ds(offset, BLOCK_K), 0:HD],
                (((1,), (1,)), ((), ())),
                preferred_element_type=jnp.float32,
            )
            first, last = first_ref[t], last_ref[t]
            parts = []
            for c in range(BLOCK_K // HD):
                position = lane + (offset + c * HD)
                visible = (position >= first) & (position <= last)
                part = jnp.where(visible, scores[:, c * HD : (c + 1) * HD], HIDDEN)
                scores_ref[index, :, c * HD : (c + 1) * HD] = part
                parts.append(part)
            top_ref[t] = jnp.maximum(top_ref[t], functools.reduce(jnp.maximum, parts))
        return carry

    lax.fori_loop(0, steps, score, 0)
    for t in range(n_tiles):
        top = top_ref[t]
        top_ref[t] = jnp.broadcast_to(jnp.max(top, axis=1, keepdims=True), top.shape)

    def weigh(i, carry):
        for u in range(UNROLL):
            index = i * UNROLL + u
            t = tile_ref[index]
            offset = pl.multiple_of(offset_ref[index], 16)
            top = top_ref[t]
            weights = [
                jnp.exp2((scores_ref[index, :, c * HD : (c + 1) * HD] - top) * factor)
                for c in range(BLOCK_K // HD)
            ]
            totals_ref[t] = totals_ref[t] + functools.reduce(jnp.add, weights)
            weights = jnp.concatenate([w.astype(jnp.bfloat16) for w in weights], axis=1)
            weighted_ref[t] = weighted_ref[t] + jnp.dot(
                weights,
                kv_ref[pl.ds(offset, BLOCK_K), HD : 2 * HD],
                preferred_element_type=jnp.float32,
            )
        return carry

    lax.fori_loop(0, steps, weigh, 0)
    for t in range(n_tiles):
        result = weighted_ref[t] / jnp.sum(totals_ref[t], axis=1, keepdims=True)
        for h in range(heads):
            o_ref[t * chunk : (t + 1) * chunk, h * HD : (h + 1) * HD] = result[
                h * chunk : (h + 1) * chunk
            ].astype(o_ref.dtype)
    weight_copy.wait()
    columns = out_refs[0].shape[1]
    width = COLUMNS
    for b in range(2 * columns // width):
        side, at = divmod(b * width, columns)
        share = jnp.dot(
            o_ref[...], w_ref[:, b * width : (b + 1) * width], preferred_element_type=jnp.float32
        ).astype(jnp.bfloat16)
        for t in range(n_tiles):
            out_refs[2 * t + side][:, at : at + width] = share[t * chunk : (t + 1) * chunk]


def attention(here, lengths, assignment, q, parts, out_weight, slots, tok_rows, lanes):
    smem = pl.BlockSpec(memory_space=pltpu.SMEM)
    vmem = pl.BlockSpec(memory_space=pltpu.VMEM)
    anywhere = pl.BlockSpec(memory_space=pl.ANY)
    all_rows = sum(part.shape[0] for part in parts)
    rows, q_width = q.shape
    chunk = rows // lanes
    stacked = q_width // HD * chunk
    n = len(slots)
    n_items = sum(min(4 * (d + 1), 28) + 1 for d in range(lanes))
    n_items = min(n_items, 29 * n) + UNROLL
    columns = out_weight.shape[1] // 2
    out = jax.ShapeDtypeStruct((chunk, columns), q.dtype)
    return pl.pallas_call(
        functools.partial(attention_kernel, slots=slots, lanes=lanes, tok_rows=tok_rows),
        out_shape=[out] * (2 * n),
        in_specs=[smem, smem, smem, vmem] + [anywhere] * (1 + len(parts)),
        out_specs=[vmem] * (2 * n),
        scratch_shapes=[
            pltpu.VMEM((all_rows, 2 * HD), q.dtype),
            pltpu.VMEM(out_weight.shape, q.dtype),
            pltpu.VMEM((n + 1, stacked, HD), q.dtype),
            pltpu.VMEM((n + 1, stacked, HD), jnp.int32),
            pltpu.VMEM((n + 1, stacked, HD), jnp.int32),
            pltpu.VMEM((n_items, stacked, BLOCK_K), jnp.float32),
            pltpu.VMEM((n + 1, stacked, HD), jnp.float32),
            pltpu.VMEM((n + 1, stacked, HD), jnp.float32),
            pltpu.VMEM((n + 1, stacked, HD), jnp.float32),
            pltpu.VMEM((n * chunk, q_width), q.dtype),
            pltpu.SMEM((n_items,), jnp.int32),
            pltpu.SMEM((n_items,), jnp.int32),
            pltpu.SemaphoreType.DMA((2 * all_rows // tok_rows,)),
            pltpu.SemaphoreType.DMA,
        ],
        cost_estimate=pl.CostEstimate(
            flops=2 * 10**9, bytes_accessed=10**7, transcendentals=2 * 10**6
        ),
        name="attention",
    )(here, lengths, assignment, q, *parts, out_weight)


def gathered(own, core):
    side = lax.axis_size("dp_0")
    half = own.shape[0] // 2

    def move(value, turn):
        pairs = []
        for y in range(side):
            for x in range(side):
                for c in range(2):
                    ty, tx, tc = turn(y, x, c)
                    target = (ty % side * side + tx % side) * 2 + tc
                    pairs.append(((y * side + x) * 2 + c, target))
        return lax.ppermute(value, DP, pairs)

    def swap(value):
        return move(value, lambda y, x, c: (y, x, 1 - c))

    def along(value, shift):
        return move(value, lambda y, x, c: (y, x + shift, c) if c == 0 else (y + shift, x, c))

    def across(value, shift):
        return move(value, lambda y, x, c: (y + shift, x, c) if c == 0 else (y, x + shift, c))

    keep = lax.dynamic_slice_in_dim(own, core * half, half, 0)
    other = swap(lax.dynamic_slice_in_dim(own, (1 - core) * half, half, 0))
    mine = jnp.where(
        core == 0,
        jnp.concatenate([keep, other], axis=0),
        jnp.concatenate([other, keep], axis=0),
    )
    row = jnp.concatenate([mine] + [along(mine, s) for s in (1, 2, 3)], axis=0)
    parts = [row] + [across(row, s) for s in (1, 2, 3)]
    return parts + [swap(part) for part in parts]


def scattered(shares, lanes):
    moving = {}
    for turn, h, j in hops(lanes):
        value = shares[j, h]
        if (turn, h) in moving:
            total = value.astype(jnp.float32) + moving[turn, h].astype(jnp.float32)
            value = total.astype(value.dtype)
        moving[turn, h] = lax.ppermute(
            value, "tensor", [(i, (i + turn) % lanes) for i in range(lanes)]
        )
    ends = []
    for h in range(2):
        total = shares[0, h].astype(jnp.float32)
        for turn in (1, -1):
            total = total + moving[turn, h].astype(jnp.float32)
        ends.append(total.astype(shares[0, h].dtype))
    return jnp.concatenate(ends, axis=1)


def hops(lanes):
    far = lanes // 2
    order = []
    for step in range(far):
        order += [(1, 0, far - step), (-1, 1, far + step)]
        if step < far - 1:
            order += [(1, 1, far - 1 - step), (-1, 0, far + 1 + step)]
    return order


def local(queries, keys, values, lengths, assignment, out_weight):
    n_groups = lax.axis_size(DP)
    lanes = lax.axis_size("tensor")
    my_group = lax.axis_index(DP)
    my_lane = lax.axis_index("tensor")
    core = lax.axis_index("dp_2")
    tok_rows, q_width = queries.shape
    piece = tok_rows // n_groups
    kv_head = my_lane * (q_width // HD) // (HEADS // KV_HEADS)
    own = jnp.concatenate(
        [lax.dynamic_slice_in_dim(a, kv_head * HD, HD, 1) for a in (keys, values)], axis=1
    )
    parts = gathered(own, core)
    outgoing = queries.reshape(n_groups, piece, q_width)[assignment[my_group]]
    q = lax.all_to_all(outgoing, DP, 0, 0, tiled=True)
    q = q.reshape(tok_rows, q_width)
    here = jnp.stack([lax.axis_index("dp_0"), lax.axis_index("dp_1"), core, my_lane])
    slots = (4, 3, 5, 2, 6, 1, 7, 0)
    outs = attention(
        here.astype(jnp.int32), lengths, assignment, q, parts, out_weight, slots, tok_rows, lanes
    )
    shares = {(slot, h): outs[2 * t + h] for t, slot in enumerate(slots) for h in range(2)}
    return scattered(shares, lanes)


def solution(mesh):
    lanes = mesh.shape["tensor"]
    split = Mesh(mesh.devices.reshape(4, 4, 2, lanes), DP_TENSOR)
    placed = (P(DP, "tensor"), P(DP, None), P(DP, None), P(), P(), P("tensor", None))

    return jax.shard_map(
        local, mesh=split, in_specs=placed, out_specs=P(DP_TENSOR, None), check_vma=False
    )
```

```python
import functools

import jax
import jax.numpy as jnp
from jax import lax
from jax.experimental import pallas as pl
from jax.experimental.pallas import tpu as pltpu
from jax.sharding import Mesh
from jax.sharding import PartitionSpec as P


HD = 128
HEADS = 24
KV_HEADS = 4
MOST = 6144
DP = ("dp_0", "dp_1", "dp_2")
DP_TENSOR = ("dp_0", "dp_1", "dp_2", "tensor")
LOG2E = 1.4426950408889634
BLOCK_K = 512
UNROLL = 12
COLUMNS = 512
VMEM_LIMIT = 60 * 1024 * 1024
HIDDEN = -2e30
FLOOR = -1e30

HELD = ((0, (0, 1, 2, 3)), (1, (0, 1, 2, 3)), (3, (0, 1, 2, 3)), (2, (0, 1)), (2, (2, 3)))


def attention_kernel(here_ref, lengths_ref, assignment_ref, q_ref, *refs, layout, lanes, tok_rows):
    sides = 4
    n_parts = 2 * len(HELD)
    part_refs, weight_ref = refs[:n_parts], refs[n_parts]
    out_refs = refs[n_parts + 1 : n_parts + 1 + len(layout)]
    scratch = refs[n_parts + 1 + len(layout) :]
    slots = range(lanes)
    kv_ref, w_ref, qs_ref, behind_ref, reach_ref, scores_ref = scratch[:6]
    top_ref, totals_ref, weighted_ref, o_ref, share_ref, tile_ref, offset_ref = scratch[6:13]
    kv_sem, w_sem, out_sem = scratch[13:]
    rows = q_ref.shape[0]
    heads = q_ref.shape[1] // HD
    all_rows = kv_ref.shape[0]
    n_groups = assignment_ref.shape[0]
    piece = rows // n_groups
    chunk = rows // lanes
    pieces = n_groups // lanes
    n_tiles = len(slots)
    factor = HD**-0.5 * LOG2E
    y, x, core, my_lane = here_ref[0], here_ref[1], here_ref[2], here_ref[3]
    group = (y * sides + x) * 2 + core

    weight_copy = pltpu.make_async_copy(weight_ref, w_ref, w_sem)
    copies = []
    for swapped in range(2):
        holder = core if swapped == 0 else 1 - core
        along = jnp.where(holder == 0, x, y)
        across = jnp.where(holder == 0, y, x)
        for n, (s, blocks) in enumerate(HELD):
            for b, r in enumerate(blocks):
                u = lax.rem(along + sides - r, sides)
                v = lax.rem(across + sides - s, sides)
                py = jnp.where(holder == 0, v, u)
                px = jnp.where(holder == 0, u, v)
                source = (py * sides + px) * 2 + holder
                start = pl.multiple_of(source * tok_rows, tok_rows)
                copies.append(
                    pltpu.make_async_copy(
                        part_refs[swapped * len(HELD) + n].at[pl.ds(b * tok_rows, tok_rows), :],
                        kv_ref.at[pl.ds(start, tok_rows), :],
                        kv_sem.at[len(copies)],
                    )
                )
    for copy in copies:
        copy.start()

    ends, at = [], jnp.int32(0)
    for k in range(lengths_ref.shape[0]):
        at = at + lengths_ref[k]
        ends.append(at)

    def place(s):
        return s * tok_rows + assignment_ref[s, group] * piece

    def doc_start(position):
        start = jnp.zeros_like(position)
        for end in ends:
            start = jnp.where(position >= end, end, start)
        return start

    row = lax.broadcasted_iota(jnp.int32, (piece, HD), 0)
    lane = lax.broadcasted_iota(jnp.int32, (piece, HD), 1)

    def fill(index, tile, offset):
        tile_ref[index] = tile
        offset_ref[index] = offset

    total = jnp.int32(0)
    for t, slot in enumerate(slots):
        owner = lax.rem(my_lane + slot, lanes)
        low = doc_start(place(owner * pieces)) // 16 * 16
        high = place(owner * pieces + pieces - 1) + piece
        count = (high - low + BLOCK_K - 1) // BLOCK_K
        low = jnp.minimum(low, all_rows - count * BLOCK_K)

        def add(i, carry, t=t, low=low, total=total):
            fill(total + i, t, low + i * BLOCK_K)
            return carry

        lax.fori_loop(0, count, add, 0)
        total = total + count
        begin = pl.multiple_of(owner * chunk, chunk)
        for h in range(heads):
            qs_ref[t, h * chunk : (h + 1) * chunk, :] = q_ref[
                pl.ds(begin, chunk), h * HD : (h + 1) * HD
            ]
        for p in range(pieces):
            position = place(owner * pieces + p) + row
            start = doc_start(position)
            for h in range(heads):
                span = pl.ds(h * chunk + p * piece, piece)
                behind_ref[t, span, :] = (lane - start).astype(jnp.uint32)
                reach_ref[t, span, :] = (position - start).astype(jnp.uint32)
    for u in range(UNROLL - 1):
        fill(total + u, n_tiles, 0)
    steps = (total + UNROLL - 1) // UNROLL
    qs_ref[n_tiles] = jnp.zeros(qs_ref.shape[1:], qs_ref.dtype)
    behind_ref[n_tiles] = jnp.zeros(behind_ref.shape[1:], jnp.uint32)
    reach_ref[n_tiles] = jnp.zeros(reach_ref.shape[1:], jnp.uint32)
    top_ref[...] = jnp.full(top_ref.shape, FLOOR, jnp.float32)
    totals_ref[...] = jnp.zeros(totals_ref.shape, jnp.float32)
    weighted_ref[...] = jnp.zeros(weighted_ref.shape, jnp.float32)
    for copy in copies:
        copy.wait()
    weight_copy.start()

    def score(i, carry):
        for u in range(UNROLL):
            index = i * UNROLL + u
            t = tile_ref[index]
            offset = pl.multiple_of(offset_ref[index], 16)
            scores = lax.dot_general(
                qs_ref[t],
                kv_ref[pl.ds(offset, BLOCK_K), 0:HD],
                (((1,), (1,)), ((), ())),
                preferred_element_type=jnp.float32,
            )
            behind, reach = behind_ref[t], reach_ref[t]
            parts = []
            for c in range(BLOCK_K // HD):
                visible = behind + (offset + c * HD).astype(jnp.uint32) <= reach
                part = jnp.where(visible, scores[:, c * HD : (c + 1) * HD], HIDDEN)
                scores_ref[index, :, c * HD : (c + 1) * HD] = part
                parts.append(part)
            top_ref[t] = jnp.maximum(top_ref[t], functools.reduce(jnp.maximum, parts))
        return carry

    lax.fori_loop(0, steps, score, 0)
    for t in range(n_tiles):
        top = top_ref[t]
        top_ref[t] = jnp.broadcast_to(jnp.max(top, axis=1, keepdims=True), top.shape)

    def weigh(i, carry):
        for u in range(UNROLL):
            index = i * UNROLL + u
            t = tile_ref[index]
            offset = pl.multiple_of(offset_ref[index], 16)
            top = top_ref[t]
            weights = [
                jnp.exp2((scores_ref[index, :, c * HD : (c + 1) * HD] - top) * factor)
                for c in range(BLOCK_K // HD)
            ]
            totals_ref[t] = totals_ref[t] + functools.reduce(jnp.add, weights)
            weights = jnp.concatenate([w.astype(jnp.bfloat16) for w in weights], axis=1)
            weighted_ref[t] = weighted_ref[t] + jnp.dot(
                weights,
                kv_ref[pl.ds(offset, BLOCK_K), HD : 2 * HD],
                preferred_element_type=jnp.float32,
            )
        return carry

    lax.fori_loop(0, steps, weigh, 0)
    for t in range(n_tiles):
        result = weighted_ref[t] / jnp.sum(totals_ref[t], axis=1, keepdims=True)
        for h in range(heads):
            o_ref[t * chunk : (t + 1) * chunk, h * HD : (h + 1) * HD] = result[
                h * chunk : (h + 1) * chunk
            ].astype(o_ref.dtype)
    weight_copy.wait()
    columns = out_refs[0].shape[1]
    width = COLUMNS

    leaving = {}
    for out_ref, held in zip(out_refs, layout):
        for n, (slot, side) in enumerate(held):
            leaving[slot, side] = pltpu.make_async_copy(
                share_ref.at[2 * slot + side],
                out_ref.at[pl.ds(n * chunk, chunk), :],
                out_sem.at[2 * slot + side],
            )

    for b in range(2 * columns // width):
        side, at = divmod(b * width, columns)
        share = jnp.dot(
            o_ref[...], w_ref[:, b * width : (b + 1) * width], preferred_element_type=jnp.float32
        ).astype(jnp.bfloat16)
        for t in range(n_tiles):
            share_ref[2 * t + side, :, at : at + width] = share[t * chunk : (t + 1) * chunk]
        if at + width == columns:
            for t in range(n_tiles):
                leaving[t, side].start()
    for copy in leaving.values():
        copy.wait()


def attention(here, lengths, assignment, q, parts, out_weight, layout, tok_rows, lanes):
    smem = pl.BlockSpec(memory_space=pltpu.SMEM)
    vmem = pl.BlockSpec(memory_space=pltpu.VMEM)
    hbm = pl.BlockSpec(memory_space=pltpu.HBM)
    all_rows = sum(part.shape[0] for part in parts)
    rows, q_width = q.shape
    chunk = rows // lanes
    stacked = q_width // HD * chunk
    n = lanes
    blocks = [pl.cdiv(min((d + 1) * rows * 4, MOST + rows * 4) + 15, BLOCK_K) for d in range(lanes)]
    n_items = sum(blocks) + UNROLL
    columns = out_weight.shape[1] // 2
    outs = [jax.ShapeDtypeStruct((chunk * len(held), columns), q.dtype) for held in layout]
    return pl.pallas_call(
        functools.partial(attention_kernel, layout=layout, lanes=lanes, tok_rows=tok_rows),
        out_shape=outs,
        in_specs=[smem, smem, smem, vmem] + [hbm] * (1 + len(parts)),
        out_specs=[hbm] * len(outs),
        scratch_shapes=[
            pltpu.VMEM((all_rows, 2 * HD), q.dtype),
            pltpu.VMEM(out_weight.shape, q.dtype),
            pltpu.VMEM((n + 1, stacked, HD), q.dtype),
            pltpu.VMEM((n + 1, stacked, HD), jnp.uint32),
            pltpu.VMEM((n + 1, stacked, HD), jnp.uint32),
            pltpu.VMEM((n_items, stacked, BLOCK_K), jnp.float32),
            pltpu.VMEM((n + 1, stacked, HD), jnp.float32),
            pltpu.VMEM((n + 1, stacked, HD), jnp.float32),
            pltpu.VMEM((n + 1, stacked, HD), jnp.float32),
            pltpu.VMEM((n * chunk, q_width), q.dtype),
            pltpu.VMEM((2 * n, chunk, columns), q.dtype),
            pltpu.SMEM((n_items,), jnp.int32),
            pltpu.SMEM((n_items,), jnp.int32),
            pltpu.SemaphoreType.DMA((all_rows // tok_rows,)),
            pltpu.SemaphoreType.DMA,
            pltpu.SemaphoreType.DMA((2 * n,)),
        ],
        cost_estimate=pl.CostEstimate(
            flops=2 * 10**9, bytes_accessed=10**7, transcendentals=2 * 10**6
        ),
        compiler_params=pltpu.CompilerParams(vmem_limit_bytes=VMEM_LIMIT),
        name="attention",
    )(here, lengths, assignment, q, *parts, out_weight)


def gathered(own, *between):
    side = lax.axis_size("dp_0")

    def move(value, turn):
        pairs = []
        for y in range(side):
            for x in range(side):
                for c in range(2):
                    ty, tx, tc = turn(y, x, c)
                    target = (ty % side * side + tx % side) * 2 + tc
                    pairs.append(((y * side + x) * 2 + c, target))
        return lax.ppermute(value, DP, pairs)

    def swap(value):
        return move(value, lambda y, x, c: (y, x, 1 - c))

    def along(value, shift):
        return move(value, lambda y, x, c: (y, x + shift, c) if c == 0 else (y + shift, x, c))

    def across(value, shift):
        return move(value, lambda y, x, c: (y + shift, x, c) if c == 0 else (y, x + shift, c))

    row = [own] + [along(own, s) for s in (1, 2, 3)]
    row, between = lax.optimization_barrier((row, between))
    row = jnp.concatenate(row, axis=0)
    half = row.shape[0] // 2
    back, front = across(row, 1), across(row, 3)
    ahead = [across(back[:half], 1), across(front[half:], 3)]
    parts = [row, back, front] + ahead
    return parts + [swap(part) for part in parts], *between


def scattered(outs, layout, lanes):
    chunk = outs[0].shape[0]
    shares = {}
    for out, held in zip(outs, layout):
        for n, (slot, h) in enumerate(held):
            shares[slot, h] = out[n * chunk : (n + 1) * chunk]
    moving = {}
    for turn, h, j in hops(lanes):
        value = shares[j, h]
        if (turn, h) in moving:
            total = value.astype(jnp.float32) + moving[turn, h].astype(jnp.float32)
            value = total.astype(value.dtype)
        moving[turn, h] = lax.ppermute(
            value, "tensor", [(i, (i + turn) % lanes) for i in range(lanes)]
        )
    terms = [[shares[0, h] for h in range(2)]]
    terms += [[moving[turn, h] for h in range(2)] for turn in (1, -1)]
    total = sum(jnp.concatenate(term, axis=1).astype(jnp.float32) for term in terms)
    return total.astype(outs[0].dtype)


def handed(lanes):
    order = [(j, h) for _, h, j in hops(lanes)]
    pairs = [tuple(order[n : n + 2]) for n in range(4, len(order), 2)]
    return tuple((one,) for one in order[:4]) + tuple(pairs) + (((0, 0),), ((0, 1),))


def hops(lanes):
    far = lanes // 2
    order = []
    for step in range(far):
        order += [(1, 0, far - step), (-1, 1, far + step)]
        if step < far - 1:
            order += [(1, 1, far - 1 - step), (-1, 0, far + 1 + step)]
    return order


def local(queries, keys, values, lengths, assignment, out_weight):
    n_groups = lax.axis_size(DP)
    lanes = lax.axis_size("tensor")
    my_group = lax.axis_index(DP)
    my_lane = lax.axis_index("tensor")
    core = lax.axis_index("dp_2")
    tok_rows, q_width = queries.shape
    piece = tok_rows // n_groups
    kv_head = my_lane * (q_width // HD) // (HEADS // KV_HEADS)
    own = jnp.concatenate(
        [lax.dynamic_slice_in_dim(a, kv_head * HD, HD, 1) for a in (keys, values)], axis=1
    )
    outgoing = queries.reshape(n_groups, piece, q_width)[assignment[my_group]]
    here = jnp.stack([lax.axis_index("dp_0"), lax.axis_index("dp_1"), core, my_lane])
    parts, outgoing, here = gathered(own, outgoing, here.astype(jnp.int32))
    q = lax.all_to_all(outgoing, DP, 0, 0, tiled=True)
    q = q.reshape(tok_rows, q_width)
    layout = handed(lanes)
    outs = attention(here, lengths, assignment, q, parts, out_weight, layout, tok_rows, lanes)
    return scattered(outs, layout, lanes)


def solution(mesh):
    lanes = mesh.shape["tensor"]
    split = Mesh(mesh.devices.reshape(4, 4, 2, lanes), DP_TENSOR)
    placed = (P(DP, "tensor"), P(DP, None), P(DP, None), P(), P(), P("tensor", None))

    return jax.shard_map(
        local, mesh=split, in_specs=placed, out_specs=P(DP_TENSOR, None), check_vma=False
    )
```
